512 devices in a mesh: rows: 32 (over y_hi, z), feat: 16 (over y_lo, x, core).
Axes of the slice: x: 4, y: 8 (y_hi: 4, y_lo: 2; y = y_hi * 2 + y_lo), z: 8, core: 2. Of those that a mesh axis runs over, the one named last changes fastest.
Arguments:
- acts: bfloat16 [32768, 8192], P('rows', 'feat'), may hold values from -6 to 6
- out_grads: bfloat16 [32768, 8192], P('rows', 'feat'), may hold values from -6 to 6
- proj_in: bfloat16 [8192, 256], P('feat'), may hold values from -0.0625 to 0.0625
- proj_out: bfloat16 [8192, 256], P('feat'), may hold values from -0.0625 to 0.0625
- assignment: int32 [32768], P('rows'), may hold values from 0 to 255
- codes: int32 [4096, 65536], P('rows', 'feat'), may hold values from -128 to 127
- zero_points: int32 [65536], P('feat'), may hold values from -64 to 63
- scales: float32 [65536], P('feat'), may hold values from 2e-06 to 2e-05
Outputs:
- scores: float32 [256, 4096], P('feat', 'rows')
The draws below stay inside these ranges and needn't reach their ends.
All inputs are finite; a program needn't handle non-finite values.
Results may differ from the reference program's by a relative error of at most 0.005.
Values may be sent and summed in bfloat16 or wider, within the bound.
No kernel may reach another device: no remote copies, remote signals or barrier semaphores. Data moves between devices by JAX's collectives and lax.ppermute only.
A program may use at most 64 MiB of HBM per device.

```python
import math
import jax
import jax.numpy as jnp
from jax import lax

D = 8192
RANK = 256
QUERIES = 256
TOK_DEV = 1024
STORE_DEV = 128
TOKENS = 32768
NSTORE = 4096
FEATURES = 65536
N_ROWS = 32


def with_ends(drawn, stream_key, low, largest):
    spot = [jax.random.randint(jax.random.fold_in(stream_key, axis), (), 0, length) for axis, length in enumerate(drawn.shape)]
    longest = drawn.shape.index(max(drawn.shape))
    beside = spot[:longest] + [(spot[longest] + 1) % drawn.shape[longest]] + spot[longest + 1:]
    return drawn.at[tuple(spot)].set(low).at[tuple(beside)].set(largest)


def block_levels(stream_key, dims, split, least, largest):
    loudness = 1.0
    for position, blocks in split:
        draws = jax.random.uniform(jax.random.fold_in(jax.random.fold_in(stream_key, 6), position), (blocks,), jnp.float32, least / len(split), largest / len(split))
        loudness = loudness * jnp.repeat(jnp.exp(draws), dims[position] // blocks).reshape((-1,) + (1,) * (len(dims) - 1 - position))
    return loudness


def centred(key, shape, width, reach, split=(), kind=jnp.bfloat16):
    gain = block_levels(key, shape, split, -0.22, 0.18) if split else 1.0
    array = jax.random.normal(key, shape, jnp.float32) * width * gain
    return jnp.minimum(jnp.maximum(array, -reach), reach).astype(kind)


def setup_inputs(seed: int = 0) -> dict:
    streams_of = jax.random.split(jax.random.key(seed), 9)
    return {
        "acts": centred(streams_of[0], (TOKENS, D), 1.0, 6.0, ((0, 32), (1, 16))),
        "out_grads": centred(streams_of[1], (TOKENS, D), 1.0, 6.0, ((0, 32), (1, 16))),
        "proj_in": centred(streams_of[2], (D, RANK), D ** -0.5, 0.0625, ((0, 16),)),
        "proj_out": centred(streams_of[3], (D, RANK), D ** -0.5, 0.0625, ((0, 16),)),
        "assignment": with_ends(jax.random.randint(streams_of[4], (TOKENS,), 0, QUERIES), jax.random.fold_in(streams_of[4], 1), 0, QUERIES - 1).astype(jnp.int32),
        "codes": with_ends(jax.random.randint(streams_of[5], (NSTORE, FEATURES), -128, 128), jax.random.fold_in(streams_of[5], 1), -128, 127).astype(jnp.int32),
        "zero_points": with_ends(jax.random.randint(streams_of[6], (FEATURES,), -64, 64), jax.random.fold_in(streams_of[6], 1), -64, 63).astype(jnp.int32),
        "scales": jnp.clip(jnp.exp(math.log(1.9999999494757503e-05) - 2.3025851 * jax.random.uniform(streams_of[7], (FEATURES,), jnp.float32) ** block_levels(streams_of[7], (FEATURES,), ((0, 16),), -0.2, 0.2)), 1.9999999949504854e-06, 1.9999999494757503e-05),
    }


def reference(acts, out_grads, proj_in, proj_out, assignment, codes, zero_points, scales):
    inner = jnp.dot(acts, proj_in, preferred_element_type=jnp.float32).astype(jnp.bfloat16)
    outer = jnp.dot(out_grads, proj_out, preferred_element_type=jnp.float32).astype(jnp.bfloat16)
    blocks = TOKENS // TOK_DEV

    def accumulate(carry, index):
        start = (index * TOK_DEV).astype(jnp.int32)
        inner_block = lax.dynamic_slice_in_dim(inner, start, TOK_DEV, 0).astype(jnp.float32)
        outer_block = lax.dynamic_slice_in_dim(outer, start, TOK_DEV, 0).astype(jnp.float32)
        owners = lax.dynamic_slice_in_dim(assignment, start, TOK_DEV, 0)
        product = (outer_block[:, :, None] * inner_block[:, None, :]).reshape(TOK_DEV, RANK * RANK)
        return carry + jax.ops.segment_sum(product, owners, num_segments=QUERIES), None

    start_grads = jnp.zeros((QUERIES, RANK * RANK), jnp.float32)
    query_grads, unused = lax.scan(accumulate, start_grads, jnp.arange(blocks, dtype=jnp.int32))
    scaled = (query_grads * scales[None, :]).astype(jnp.bfloat16)
    store_blocks = codes.reshape(N_ROWS, STORE_DEV, RANK * RANK)

    def score_block(block_codes):
        levels = (block_codes - zero_points[None, :]).astype(jnp.bfloat16)
        return lax.dot_general(scaled, levels, (((1,), (1,)), ((), ())), preferred_element_type=jnp.float32)

    parts = lax.map(score_block, store_blocks)
    return jnp.transpose(parts, (1, 0, 2)).reshape(QUERIES, NSTORE)
```

```python
import jax
import jax.numpy as jnp
from jax import lax
from jax.experimental import pallas as pl
from jax.experimental.pallas import tpu as pltpu
from jax.sharding import Mesh
from jax.sharding import PartitionSpec as P

RANK = 256
QUERIES = 256
AXES = ("yh", "z", "yl", "x", "c")
ROWS = ("yh", "z")
FEAT = ("yl", "x", "c")
NZ = 8
NW = 8
NF = 16
NI = 16
NJ = 32
LINK_GAIN = 256.0
f32 = jnp.float32
bf16 = jnp.bfloat16
f16 = jnp.float16


def exchange(blocks, axes):
    return lax.all_to_all(blocks, axes, 0, 0, tiled=True)


def spread(block, axes, size):
    return exchange(jnp.broadcast_to(block[None], (size, *block.shape)), axes)


def store_kernel(codes_ref, zero_ref, out_ref):
    for i in range(codes_ref.shape[1] // RANK):
        cols = slice(i * RANK, (i + 1) * RANK)
        levels = (codes_ref[:, cols] - zero_ref[:, cols]).astype(f32)
        out_ref[:, i, :, :] = levels.T.astype(bf16).reshape(NZ, NJ, levels.shape[0])


def store_levels(codes, zero_points):
    rows = codes.shape[0]
    step = 4
    return pl.pallas_call(
        store_kernel,
        grid=(NI // step,),
        in_specs=[
            pl.BlockSpec((rows, step * RANK), lambda g: (0, g)),
            pl.BlockSpec((1, step * RANK), lambda g: (0, g)),
        ],
        out_specs=pl.BlockSpec((NZ, step, NJ, rows), lambda g: (0, g, 0, 0)),
        out_shape=jax.ShapeDtypeStruct((NZ, NI, NJ, rows), bf16),
        name="store_levels",
    )(codes, zero_points.reshape(1, -1))


def grads_kernel(inner_ref, outer_ref, scale_ref, out_ref, acc):
    acc[...] = jnp.zeros_like(acc)
    half = inner_ref.shape[2]
    query = lax.broadcasted_iota(jnp.int32, (QUERIES, half), 0).astype(f32)

    def row(r, carry):
        owners = outer_ref[r, 2 * NI : 2 * NI + 8, :].astype(f32)
        for h in range(2):
            outer = outer_ref[r, h * NI : (h + 1) * NI, :].astype(f32)
            inner = inner_ref[2 * r + h].astype(f32)
            product = (outer[:, None, :] * inner[None, :, :]).reshape(NI * NJ, half)
            high = product.astype(bf16)
            low = (product - high.astype(f32)).astype(bf16)
            mine = jnp.where(query == owners[h : h + 1, :], 1.0, 0.0).astype(bf16)
            dims = (((1,), (1,)), ((), ()))
            acc[...] += lax.dot_general(high, mine, dims, preferred_element_type=f32) + lax.dot_general(
                low, mine, dims, preferred_element_type=f32
            )
        return carry

    lax.fori_loop(0, NZ, row, 0)
    out_ref[...] = (acc[...].T * scale_ref[...]).astype(bf16)


def query_grads(inner, outer, scale):
    return pl.pallas_call(
        grads_kernel,
        in_specs=[pl.BlockSpec(memory_space=pltpu.VMEM)] * 3,
        out_specs=pl.BlockSpec(memory_space=pltpu.VMEM),
        out_shape=jax.ShapeDtypeStruct((QUERIES, NI * NJ), bf16),
        scratch_shapes=[pltpu.VMEM((NI * NJ, QUERIES), f32)],
        name="query_grads",
    )(inner, outer, scale)


def terms_kernel(core_ref, scaled_ref, store_ref, keep_ref, send_ref):
    me = core_ref[0]
    for r in range(NZ):
        terms = jnp.dot(scaled_ref[...], store_ref[r], preferred_element_type=f32)
        terms = terms.reshape(NW, 2, QUERIES // NF, terms.shape[1])
        first, second = terms[:, 0], terms[:, 1]
        keep_ref[r] = jnp.where(me == 0, first, second)
        send_ref[r] = jnp.where(me == 0, second, first)


def score_terms(core, scaled, store):
    shape = jax.ShapeDtypeStruct((NZ, NW, QUERIES // NF, store.shape[2]), f32)
    return pl.pallas_call(
        terms_kernel,
        in_specs=[pl.BlockSpec(memory_space=pltpu.SMEM)] + [pl.BlockSpec(memory_space=pltpu.VMEM)] * 2,
        out_specs=[pl.BlockSpec(memory_space=pltpu.VMEM)] * 2,
        out_shape=[shape, shape],
        name="score_terms",
    )(core, scaled, store)


def local(acts, out_grads, proj_in, proj_out, assignment, codes, zero_points, scales):
    tokens = acts.shape[0]
    half = tokens // 2
    z = lax.axis_index("z")
    dims = (((0,), (1,)), ((), ()))
    part_inner = lax.dot_general(proj_in, acts, dims, preferred_element_type=f32) * LINK_GAIN
    part_outer = lax.dot_general(proj_out, out_grads, dims, preferred_element_type=f32) * LINK_GAIN
    send_inner = part_inner.astype(f16).reshape(NW, NJ, 2, half).transpose(0, 2, 1, 3)
    send_inner = send_inner.reshape(NF, NJ, half)
    send_outer = part_outer.astype(f16).reshape(NF, NI, tokens)
    inner_terms = exchange(send_inner, FEAT)
    outer_terms = exchange(send_outer, FEAT)
    inner = (jnp.sum(inner_terms.astype(f32), axis=0) * (1.0 / LINK_GAIN)).astype(bf16)
    outer = (jnp.sum(outer_terms.astype(f32), axis=0) * (1.0 / LINK_GAIN)).astype(bf16)

    swap = [((r * NW + w) , (w * NW + r)) for r in range(NZ) for w in range(NW)]
    inner = lax.ppermute(inner, ("z", "yl", "x"), swap)
    inner_all = spread(inner, FEAT, NF)

    outer = outer.reshape(NI, 2, half).transpose(1, 0, 2).reshape(2 * NI, half)
    owners = assignment.reshape(2, half).astype(bf16)
    outer = jnp.concatenate([outer, owners, jnp.zeros((6, half), bf16)], axis=0)
    outer_all = spread(outer, "z", NZ)

    store = store_levels(codes, zero_points).reshape(NZ, NI * NJ, codes.shape[0])
    store_all = exchange(store, "z")

    scale = lax.dynamic_slice_in_dim(scales.reshape(NI, NZ, NJ), z, 1, 1).reshape(1, NI * NJ)
    grads = query_grads(inner_all, outer_all, scale)
    grad_terms = exchange(grads.reshape(4, QUERIES // 4, NI * NJ), "yh")
    share = jnp.sum(grad_terms.astype(f32), axis=0).astype(bf16)
    scaled = spread(share, "yh", 4).reshape(QUERIES, NI * NJ)

    core = lax.axis_index("c").reshape(1).astype(jnp.int32)
    keep, send = score_terms(core, scaled, store_all)
    got = lax.ppermute(send, "c", [(0, 1), (1, 0)])
    terms = (keep + got).astype(bf16).reshape(NZ * NW, QUERIES // NF, codes.shape[0])
    terms = exchange(terms, ("z", "yl", "x"))
    return jnp.sum(terms.astype(f32), axis=0)


def solution(mesh):
    split = Mesh(mesh.devices.reshape(4, 8, 2, 4, 2), AXES)
    in_specs = (
        P(ROWS, FEAT),
        P(ROWS, FEAT),
        P(FEAT, None),
        P(FEAT, None),
        P(ROWS),
        P(ROWS, FEAT),
        P(FEAT),
        P(FEAT),
    )
    out_specs = P(FEAT, ROWS)
    return jax.shard_map(local, mesh=split, in_specs=in_specs, out_specs=out_specs, check_vma=False)
```

```python
import jax
import jax.numpy as jnp
from jax import lax
from jax.experimental import pallas as pl
from jax.experimental.pallas import tpu as pltpu
from jax.sharding import Mesh
from jax.sharding import PartitionSpec as P


RANK = 256
QUERIES = 256
AXES = ("yh", "z", "yl", "x", "c")
ROWS = ("yh", "z")
FEAT = ("yl", "x", "c")
NY = 4
NZ = 8
NW = 8
NF = 16
NI = 16
NJ = 16
HALF = NI * NJ
LANES = 128
OWNER_ROW = 128
PACKED_ROWS = 144
LINK_GAIN = 256.0
f32 = jnp.float32
bf16 = jnp.bfloat16
f16 = jnp.float16
VMEM = pl.BlockSpec(memory_space=pltpu.VMEM)
SMEM = pl.BlockSpec(memory_space=pltpu.SMEM)
SMALL = pltpu.CompilerParams(vmem_limit_bytes=16 * 2**20)


def exchange(blocks, axes):
    return lax.all_to_all(blocks, axes, 0, 0, tiled=True)


def store_kernel(place_ref, codes_ref, zero_ref, *refs):
    outs, turned = refs[:NZ], refs[NZ]
    z, c = place_ref[0], place_ref[1]
    for i in range(codes_ref.shape[1] // RANK):
        cols = slice(i * RANK, (i + 1) * RANK)
        turned[...] = (codes_ref[:, cols] - zero_ref[:, cols]).astype(f32).T
        for k in range(NZ):
            for s in range(2):
                first = pl.multiple_of((((z + k) & (NZ - 1)) * 2 + (c ^ s)) * NJ, NJ)
                outs[k][s, i * NJ : (i + 1) * NJ, :] = turned[pl.ds(first, NJ), :].astype(bf16)


def store_levels(place, codes, zero_points):
    rows = codes.shape[0]
    step = 4
    return pl.pallas_call(
        store_kernel,
        grid=(NI // step,),
        in_specs=[
            SMEM,
            pl.BlockSpec((rows, step * RANK), lambda g: (0, g)),
            pl.BlockSpec((1, step * RANK), lambda g: (0, g)),
        ],
        out_specs=[pl.BlockSpec((2, step * NJ, rows), lambda g: (0, g, 0))] * NZ,
        out_shape=[jax.ShapeDtypeStruct((2, HALF, rows), bf16)] * NZ,
        scratch_shapes=[pltpu.VMEM((RANK, rows), f32)],
        compiler_params=SMALL,
        name="store_levels",
    )(place, codes, zero_points.reshape(1, -1))


def pack_kernel(sums_ref, owner_ref, inner_ref, packed_ref):
    values = sums_ref[...] * (1.0 / LINK_GAIN)
    inner_ref[...] = values[:NJ].astype(bf16)
    outer = values[NJ:].astype(bf16)
    owners = owner_ref[...].astype(f32)
    tail = jnp.concatenate([owners, jnp.zeros_like(owners)], axis=0).astype(bf16)
    for r in range(NZ):
        for t in range(NZ):
            packed_ref[r, t * NI : (t + 1) * NI, :] = outer[:, t * LANES : (t + 1) * LANES]
        packed_ref[r, OWNER_ROW:, :] = tail


def pack_tokens(sums, assignment):
    return pl.pallas_call(
        pack_kernel,
        in_specs=[VMEM] * 2,
        out_specs=[VMEM] * 2,
        out_shape=[
            jax.ShapeDtypeStruct((NJ, sums.shape[1]), bf16),
            jax.ShapeDtypeStruct((NZ, PACKED_ROWS, LANES), bf16),
        ],
        compiler_params=SMALL,
        name="pack_tokens",
    )(sums, assignment.reshape(NZ, LANES))


def grads_kernel(inner_ref, own_ref, other_ref, scale_ref, out_ref, acc):
    acc[...] = jnp.zeros_like(acc)
    tiles = 4
    span = tiles * LANES
    query = lax.broadcasted_iota(jnp.int32, (QUERIES, span), 0).astype(f32)

    def row(r, carry):
        owners = own_ref[r, OWNER_ROW:, :].astype(f32)
        for p in range(NZ // tiles):
            inner = inner_ref[r, :, p * span : (p + 1) * span].astype(f32)
            cut = range(p * tiles, (p + 1) * tiles)
            parts = []
            for ref in (own_ref, other_ref):
                outer = jnp.concatenate([ref[r, t * NI : (t + 1) * NI, :] for t in cut], axis=1).astype(f32)
                parts.append((outer[:, None, :] * inner[None, :, :]).reshape(HALF, span).astype(bf16))
            product = jnp.concatenate(parts, axis=0)
            owner = jnp.concatenate([owners[t : t + 1, :] for t in cut], axis=1)
            mine = jnp.where(query == owner, 1.0, 0.0).astype(bf16)
            acc[...] += lax.dot_general(product, mine, (((1,), (1,)), ((), ())), preferred_element_type=f32)
        return carry

    lax.fori_loop(0, NZ, row, 0)
    out_ref[...] = (acc[...].T * scale_ref[...]).astype(bf16)


def query_grads(inner, own, other, scale):
    return pl.pallas_call(
        grads_kernel,
        in_specs=[VMEM] * 4,
        out_specs=VMEM,
        out_shape=jax.ShapeDtypeStruct((QUERIES, 2 * HALF), bf16),
        scratch_shapes=[pltpu.VMEM((2 * HALF, QUERIES), f32)],
        compiler_params=SMALL,
        name="query_grads",
    )(inner, own, other, scale)


def share_kernel(terms_ref, out_ref):
    total = terms_ref[0].astype(f32)
    for y in range(1, NY):
        total += terms_ref[y].astype(f32)
    share = total.astype(bf16)
    for y in range(NY):
        out_ref[y] = share


def spread_share(terms):
    return pl.pallas_call(
        share_kernel,
        in_specs=[VMEM],
        out_specs=VMEM,
        out_shape=jax.ShapeDtypeStruct(terms.shape, bf16),
        compiler_params=SMALL,
        name="spread_share",
    )(terms)


def terms_kernel(place_ref, scaled_ref, other_ref, *refs):
    own, (keep_ref, send_ref) = refs[:NZ], refs[NZ:]
    z, c = place_ref[0], place_ref[1]
    for k in range(NZ):
        terms = jnp.dot(scaled_ref[:, :HALF], own[k][0], preferred_element_type=f32)
        terms += jnp.dot(scaled_ref[:, HALF:], other_ref[k], preferred_element_type=f32)
        terms = terms.reshape(NW, 2, QUERIES // NF, terms.shape[1])
        first, second = terms[:, 0], terms[:, 1]
        r = (z + NZ - k) & (NZ - 1)
        keep_ref[r] = jnp.where(c == 0, first, second)
        send_ref[r] = jnp.where(c == 0, second, first)


def score_terms(place, scaled, own, other):
    shape = jax.ShapeDtypeStruct((NZ, NW, QUERIES // NF, other.shape[2]), f32)
    return pl.pallas_call(
        terms_kernel,
        in_specs=[SMEM] + [VMEM] * (2 + NZ),
        out_specs=[VMEM] * 2,
        out_shape=[shape, shape],
        compiler_params=SMALL,
        name="score_terms",
    )(place, scaled, other, *own)


def local(acts, out_grads, proj_in, proj_out, assignment, codes, zero_points, scales):
    tokens = acts.shape[0]
    z = lax.axis_index("z")
    c = lax.axis_index("c")
    place = jnp.stack([z, c]).astype(jnp.int32)
    flip = [(0, 1), (1, 0)]

    dims = (((0,), (1,)), ((), ()))
    part_inner = lax.dot_general(proj_in, acts, dims, preferred_element_type=f32) * LINK_GAIN
    part_outer = lax.dot_general(proj_out, out_grads, dims, preferred_element_type=f32) * LINK_GAIN
    part_inner = part_inner.astype(f16).reshape(NF, NJ, tokens)
    part_outer = part_outer.astype(f16).reshape(NF, NI, tokens)
    parts = exchange(jnp.concatenate([part_inner, part_outer], axis=1), FEAT)
    sums = jnp.sum(parts.astype(f32), axis=0)

    inner, packed = pack_tokens(sums, assignment)
    own = exchange(packed, "z")
    swap = [(r * NW + w, w * NW + r) for r in range(NZ) for w in range(NW)]
    inner = lax.ppermute(inner, ("z", "yl", "x"), swap)
    inner = exchange(jnp.broadcast_to(inner[None], (NW, *inner.shape)), ("yl", "x"))
    other = lax.ppermute(own, "c", flip)

    store = store_levels(place, codes, zero_points)
    store = [lax.ppermute(store[k], "z", [(r, (r + k) % NZ) for r in range(NZ)]) if k else store[0] for k in range(NZ)]
    store_other = lax.ppermute(jnp.stack([block[1] for block in store]), "c", flip)

    scales = scales.reshape(NI, NF, NJ)
    own_scale = lax.dynamic_slice_in_dim(scales, z * 2 + c, 1, 1).reshape(NI, NJ)
    other_scale = lax.dynamic_slice_in_dim(scales, z * 2 + 1 - c, 1, 1).reshape(NI, NJ)
    other_scale = lax.ppermute(other_scale, "c", flip)
    scale = jnp.concatenate([own_scale, other_scale], axis=0).reshape(1, 2 * HALF)

    grads = query_grads(inner, own, other, scale)
    grads = exchange(grads.reshape(NY, QUERIES // NY, 2 * HALF), "yh")
    scaled = exchange(spread_share(grads), "yh").reshape(QUERIES, 2 * HALF)

    keep, send = score_terms(place, scaled, store, store_other)
    got = lax.ppermute(send, "c", flip)
    terms = (keep + got).astype(bf16).reshape(NZ * NW, QUERIES // NF, codes.shape[0])
    terms = exchange(terms, ("z", "yl", "x"))
    return jnp.sum(terms.astype(f32), axis=0)


def solution(mesh):
    split = Mesh(mesh.devices.reshape(4, 8, 2, 4, 2), AXES)
    in_specs = (
        P(ROWS, FEAT),
        P(ROWS, FEAT),
        P(FEAT, None),
        P(FEAT, None),
        P(ROWS),
        P(ROWS, FEAT),
        P(FEAT),
        P(FEAT),
    )
    out_specs = P(FEAT, ROWS)
    return jax.shard_map(local, mesh=split, in_specs=in_specs, out_specs=out_specs, check_vma=False)
```

```python
import jax
import jax.numpy as jnp
from jax import lax
from jax.experimental import pallas as pl
from jax.experimental.pallas import tpu as pltpu
from jax.sharding import Mesh
from jax.sharding import PartitionSpec as P


RANK = 256
QUERIES = 256
AXES = ("yh", "zh", "zl", "yl", "x", "c")
ROWS = ("yh", "zh", "zl")
FEAT = ("yl", "x", "c")
NY = 4
NZ = 8
ZH = 2
ZL = 4
NW = 8
NF = 16
NI = 16
NJ = 16
HALF = NI * NJ
LANES = 128
OWNER_ROW = 128
PACKED_ROWS = 144
LINK_GAIN = 256.0
f32 = jnp.float32
bf16 = jnp.bfloat16
f16 = jnp.float16
VMEM = pl.BlockSpec(memory_space=pltpu.VMEM)
SMEM = pl.BlockSpec(memory_space=pltpu.SMEM)
SMALL = pltpu.CompilerParams(vmem_limit_bytes=16 * 2**20)


def exchange(blocks, axes):
    return lax.all_to_all(blocks, axes, 0, 0, tiled=True)


def store_kernel(place_ref, codes_ref, zero_ref, *refs):
    outs, turned = refs[:ZL], refs[ZL]
    zl, c = place_ref[0], place_ref[1]
    for i in range(codes_ref.shape[1] // RANK):
        cols = slice(i * RANK, (i + 1) * RANK)
        turned[...] = (codes_ref[:, cols] - zero_ref[:, cols]).astype(f32).T
        for k in range(ZL):
            for s in range(2):
                for h in range(ZH):
                    block = (h * ZL + (zl ^ k)) * 2 + (c ^ s)
                    rows = pl.ds(pl.multiple_of(block * NJ, NJ), NJ)
                    outs[k][s, h, i * NJ : (i + 1) * NJ, :] = turned[rows, :].astype(bf16)


def store_levels(place, codes, zero_points):
    rows = codes.shape[0]
    step = 4
    return pl.pallas_call(
        store_kernel,
        grid=(NI // step,),
        in_specs=[
            SMEM,
            pl.BlockSpec((rows, step * RANK), lambda g: (0, g)),
            pl.BlockSpec((1, step * RANK), lambda g: (0, g)),
        ],
        out_specs=[pl.BlockSpec((2, ZH, step * NJ, rows), lambda g: (0, 0, g, 0))] * ZL,
        out_shape=[jax.ShapeDtypeStruct((2, ZH, HALF, rows), bf16)] * ZL,
        scratch_shapes=[pltpu.VMEM((RANK, rows), f32)],
        compiler_params=SMALL,
        name="store_levels",
    )(place, codes, zero_points.reshape(1, -1))


def pick_kernel(place_ref, scales_ref, own_ref, other_ref):
    c, z = place_ref[1], place_ref[2]
    own_ref[...] = scales_ref[:, pl.ds(z * 2 + c, 1), :]
    other_ref[...] = scales_ref[:, pl.ds(z * 2 + 1 - c, 1), :]


def pick_scales(place, scales):
    return pl.pallas_call(
        pick_kernel,
        in_specs=[SMEM, VMEM],
        out_specs=[VMEM] * 2,
        out_shape=[jax.ShapeDtypeStruct((NI, 1, NJ), f32)] * 2,
        compiler_params=SMALL,
        name="pick_scales",
    )(place, scales.reshape(NI, NF, NJ))


def pack_kernel(sums_ref, owner_ref, inner_ref, packed_ref):
    values = sums_ref[...] * (1.0 / LINK_GAIN)
    inner_ref[...] = values[:NJ].astype(bf16)
    outer = values[NJ:].astype(bf16)
    owners = owner_ref[...].astype(f32)
    tail = jnp.concatenate([owners, jnp.zeros_like(owners)], axis=0).astype(bf16)
    for r in range(NZ):
        for t in range(NZ):
            packed_ref[r, t * NI : (t + 1) * NI, :] = outer[:, t * LANES : (t + 1) * LANES]
        packed_ref[r, OWNER_ROW:, :] = tail


def pack_tokens(sums, assignment):
    return pl.pallas_call(
        pack_kernel,
        in_specs=[VMEM] * 2,
        out_specs=[VMEM] * 2,
        out_shape=[
            jax.ShapeDtypeStruct((NJ, sums.shape[1]), bf16),
            jax.ShapeDtypeStruct((NZ, PACKED_ROWS, LANES), bf16),
        ],
        compiler_params=SMALL,
        name="pack_tokens",
    )(sums, assignment.reshape(NZ, LANES))


def grads_kernel(inner_ref, own_ref, other_ref, scale_ref, out_ref, acc):
    acc[...] = jnp.zeros_like(acc)
    tiles = 4
    span = tiles * LANES
    query = lax.broadcasted_iota(jnp.int32, (QUERIES, span), 0).astype(f32)

    def row(r, carry):
        owners = own_ref[r, OWNER_ROW:, :].astype(f32)
        for p in range(NZ // tiles):
            inner = inner_ref[r, :, p * span : (p + 1) * span].astype(f32)
            cut = range(p * tiles, (p + 1) * tiles)
            parts = []
            for ref in (own_ref, other_ref):
                outer = jnp.concatenate([ref[r, t * NI : (t + 1) * NI, :] for t in cut], axis=1).astype(f32)
                parts.append((outer[:, None, :] * inner[None, :, :]).reshape(HALF, span).astype(bf16))
            product = jnp.concatenate(parts, axis=0)
            owner = jnp.concatenate([owners[t : t + 1, :] for t in cut], axis=1)
            mine = jnp.where(query == owner, 1.0, 0.0).astype(bf16)
            acc[...] += lax.dot_general(product, mine, (((1,), (1,)), ((), ())), preferred_element_type=f32)
        return carry

    lax.fori_loop(0, NZ, row, 0)
    out_ref[...] = (acc[...].T * scale_ref[...]).astype(bf16)


def query_grads(inner, own, other, scale):
    return pl.pallas_call(
        grads_kernel,
        in_specs=[VMEM] * 4,
        out_specs=VMEM,
        out_shape=jax.ShapeDtypeStruct((QUERIES, 2 * HALF), bf16),
        scratch_shapes=[pltpu.VMEM((2 * HALF, QUERIES), f32)],
        compiler_params=SMALL,
        name="query_grads",
    )(inner, own, other, scale)


def share_kernel(terms_ref, out_ref):
    total = terms_ref[0].astype(f32)
    for y in range(1, NY):
        total += terms_ref[y].astype(f32)
    share = total.astype(bf16)
    for y in range(NY * ZH):
        out_ref[y] = share


def spread_share(terms):
    return pl.pallas_call(
        share_kernel,
        in_specs=[VMEM],
        out_specs=VMEM,
        out_shape=jax.ShapeDtypeStruct((NY * ZH, *terms.shape[1:]), bf16),
        compiler_params=SMALL,
        name="spread_share",
    )(terms)


def terms_kernel(place_ref, scaled_ref, other_ref, *refs):
    own, (keep_ref, send_ref) = refs[:ZL], refs[ZL:]
    zl, c = place_ref[0], place_ref[1]
    for k in range(ZL):
        terms = jnp.zeros((QUERIES, other_ref.shape[3]), f32)
        for h in range(ZH):
            terms += jnp.dot(scaled_ref[h, :, :HALF], own[k][0, h], preferred_element_type=f32)
            terms += jnp.dot(scaled_ref[h, :, HALF:], other_ref[k, h], preferred_element_type=f32)
        terms = terms.reshape(NW, 2, QUERIES // NF, terms.shape[1])
        first, second = terms[:, 0], terms[:, 1]
        keep_ref[zl ^ k] = jnp.where(c == 0, first, second)
        send_ref[zl ^ k] = jnp.where(c == 0, second, first)


def score_terms(place, scaled, own, other):
    shape = jax.ShapeDtypeStruct((ZL, NW, QUERIES // NF, other.shape[3]), f32)
    return pl.pallas_call(
        terms_kernel,
        in_specs=[SMEM] + [VMEM] * (2 + ZL),
        out_specs=[VMEM] * 2,
        out_shape=[shape, shape],
        compiler_params=SMALL,
        name="score_terms",
    )(place, scaled, other, *own)


def local(acts, out_grads, proj_in, proj_out, assignment, codes, zero_points, scales):
    tokens = acts.shape[0]
    zl = lax.axis_index("zl")
    z = lax.axis_index("zh") * ZL + zl
    c = lax.axis_index("c")
    place = jnp.stack([zl, c, z]).astype(jnp.int32)
    flip = [(0, 1), (1, 0)]

    dims = (((0,), (1,)), ((), ()))
    part_inner = lax.dot_general(proj_in, acts, dims, preferred_element_type=f32) * LINK_GAIN
    part_outer = lax.dot_general(proj_out, out_grads, dims, preferred_element_type=f32) * LINK_GAIN
    part_inner = part_inner.astype(f16).reshape(NF, NJ, tokens)
    part_outer = part_outer.astype(f16).reshape(NF, NI, tokens)
    parts = exchange(jnp.concatenate([part_inner, part_outer], axis=1), FEAT)
    sums = jnp.sum(parts.astype(f32), axis=0)

    inner, packed = pack_tokens(sums, assignment)
    own = exchange(packed, ("zh", "zl"))
    swap = [(r * NW + w, w * NW + r) for r in range(NZ) for w in range(NW)]
    inner_swapped = lax.ppermute(inner, ("zh", "zl", "yl", "x"), swap)
    inner_all = exchange(jnp.broadcast_to(inner_swapped[None], (NW, *inner.shape)), ("yl", "x"))
    other = lax.ppermute(own, "c", flip)

    store = list(store_levels(place, codes, zero_points))
    for k in range(1, ZL):
        store[k] = lax.ppermute(store[k], "zl", [(r, r ^ k) for r in range(ZL)])
    store_other = lax.ppermute(jnp.stack([block[1] for block in store]), "c", flip)

    own_scale, other_scale = pick_scales(place, scales)
    other_scale = lax.ppermute(other_scale, "c", flip)
    scale = jnp.concatenate([own_scale, other_scale], axis=0).reshape(1, 2 * HALF)

    grads = query_grads(inner_all, own, other, scale)
    grads = exchange(grads.reshape(NY, QUERIES // NY, 2 * HALF), "yh")
    scaled = exchange(spread_share(grads), ("zh", "yh")).reshape(ZH, QUERIES, 2 * HALF)

    keep, send = score_terms(place, scaled, store, store_other)
    got = lax.ppermute(send, "c", flip)
    terms = (keep + got).astype(bf16).reshape(ZL * NW, QUERIES // NF, codes.shape[0])
    terms = exchange(terms, ("zl", "yl", "x"))
    return jnp.sum(terms.astype(f32), axis=0)


def solution(mesh):
    split = Mesh(mesh.devices.reshape(4, 2, 4, 2, 4, 2), AXES)
    in_specs = (
        P(ROWS, FEAT),
        P(ROWS, FEAT),
        P(FEAT, None),
        P(FEAT, None),
        P(ROWS),
        P(ROWS, FEAT),
        P(FEAT),
        P(FEAT),
    )
    out_specs = P(FEAT, ROWS)
    return jax.shard_map(local, mesh=split, in_specs=in_specs, out_specs=out_specs, check_vma=False)
```

```python
import jax
import jax.numpy as jnp
from jax import lax
from jax.experimental import pallas as pl
from jax.experimental.pallas import tpu as pltpu
from jax.sharding import Mesh
from jax.sharding import PartitionSpec as P


RANK = 256
QUERIES = 256
AXES = ("yh", "zl", "zh", "yl", "x", "c")
ROWS = ("yh", "zl", "zh")
FEAT = ("yl", "x", "c")
NY = 4
NZ = 8
ZH = 2
ZL = 4
NW = 8
NF = 16
NI = 16
NJ = 16
HALF = NI * NJ
LANES = 128
OWNER_ROW = 128
PACKED_ROWS = 144
LINK_GAIN = 128.0
f32 = jnp.float32
bf16 = jnp.bfloat16
f16 = jnp.float16
VMEM = pl.BlockSpec(memory_space=pltpu.VMEM)
SMEM = pl.BlockSpec(memory_space=pltpu.SMEM)
SMALL = pltpu.CompilerParams(vmem_limit_bytes=16 * 2**20)


def exchange(blocks, axes):
    return lax.all_to_all(blocks, axes, 0, 0, tiled=True)


def store_kernel(place_ref, codes_ref, zero_ref, *refs):
    outs, turned = refs[:ZL], refs[ZL]
    zl, c = place_ref[0], place_ref[1]
    for i in range(codes_ref.shape[1] // RANK):
        cols = slice(i * RANK, (i + 1) * RANK)
        turned[...] = (codes_ref[:, cols] - zero_ref[:, cols]).astype(f32).T
        for k in range(ZL):
            for s in range(2):
                for h in range(ZH):
                    block = (c ^ s) * NZ + (zl ^ k) * ZH + h
                    rows = pl.ds(pl.multiple_of(block * NJ, NJ), NJ)
                    outs[k][s, h, i * NJ : (i + 1) * NJ, :] = turned[rows, :].astype(bf16)


def store_levels(place, codes, zero_points):
    rows = codes.shape[0]
    step = 4
    return pl.pallas_call(
        store_kernel,
        grid=(NI // step,),
        in_specs=[
            SMEM,
            pl.BlockSpec((rows, step * RANK), lambda g: (0, g)),
            pl.BlockSpec((1, step * RANK), lambda g: (0, g)),
        ],
        out_specs=[pl.BlockSpec((2, ZH, step * NJ, rows), lambda g: (0, 0, g, 0))] * ZL,
        out_shape=[jax.ShapeDtypeStruct((2, ZH, HALF, rows), bf16)] * ZL,
        scratch_shapes=[pltpu.VMEM((RANK, rows), f32)],
        compiler_params=SMALL,
        name="store_levels",
    )(place, codes, zero_points.reshape(1, -1))


def pick_kernel(place_ref, scales_ref, own_ref, other_ref):
    c, z = place_ref[1], place_ref[2]
    own_ref[...] = scales_ref[:, pl.ds(c * NZ + z, 1), :]
    other_ref[...] = scales_ref[:, pl.ds((1 - c) * NZ + z, 1), :]


def pick_scales(place, scales):
    return pl.pallas_call(
        pick_kernel,
        in_specs=[SMEM, VMEM],
        out_specs=[VMEM] * 2,
        out_shape=[jax.ShapeDtypeStruct((NI, 1, NJ), f32)] * 2,
        compiler_params=SMALL,
        name="pick_scales",
    )(place, scales.reshape(NI, NF, NJ))


def project_kernel(place_ref, acts_ref, grads_ref, in_ref, out_ref, keep_ref, send_ref, turned, full):
    c = place_ref[1]

    @pl.when(pl.program_id(0) == 0)
    def turn():
        turned[0] = in_ref[...].T
        turned[1] = out_ref[...].T

    for side, ref in enumerate((acts_ref, grads_ref)):
        full[side] = lax.dot_general(
            turned[side], ref[...], (((1,), (1,)), ((), ())), preferred_element_type=f32
        )
    for w in range(NW):
        for ref, core in ((keep_ref, c), (send_ref, 1 - c)):
            rows = pl.ds(pl.multiple_of((core * NZ + w) * NJ, NJ), NJ)
            ref[w, :NJ, :] = full[0, rows, :]
            rows = pl.ds(pl.multiple_of((w * 2 + core) * NI, NI), NI)
            ref[w, NJ:, :] = full[1, rows, :]


def project(place, acts, out_grads, proj_in, proj_out):
    tokens, depth = acts.shape
    span = 2 * LANES
    wide = pl.BlockSpec((span, depth), lambda g: (g, 0))
    whole = pl.BlockSpec((depth, RANK), lambda g: (0, 0))
    shape = jax.ShapeDtypeStruct((NW, NJ + NI, tokens), f32)
    return pl.pallas_call(
        project_kernel,
        grid=(tokens // span,),
        in_specs=[SMEM, wide, wide, whole, whole],
        out_specs=[pl.BlockSpec((NW, NJ + NI, span), lambda g: (0, 0, g))] * 2,
        out_shape=[shape] * 2,
        scratch_shapes=[pltpu.VMEM((2, RANK, depth), bf16), pltpu.VMEM((2, RANK, span), f32)],
        name="project",
    )(place, acts, out_grads, proj_in, proj_out)


def pack_kernel(sums_ref, owner_ref, inner_ref, packed_ref):
    values = sums_ref[...] * (1.0 / LINK_GAIN)
    inner_ref[...] = values[:NJ].astype(bf16)
    outer = values[NJ:].astype(bf16)
    owners = owner_ref[...].astype(f32)
    tail = jnp.concatenate([owners, jnp.zeros_like(owners)], axis=0).astype(bf16)
    for r in range(NZ):
        for t in range(NZ):
            packed_ref[r, t * NI : (t + 1) * NI, :] = outer[:, t * LANES : (t + 1) * LANES]
        packed_ref[r, OWNER_ROW:, :] = tail


def pack_tokens(sums, assignment):
    return pl.pallas_call(
        pack_kernel,
        in_specs=[VMEM] * 2,
        out_specs=[VMEM] * 2,
        out_shape=[
            jax.ShapeDtypeStruct((NJ, sums.shape[1]), bf16),
            jax.ShapeDtypeStruct((NZ, PACKED_ROWS, LANES), bf16),
        ],
        compiler_params=SMALL,
        name="pack_tokens",
    )(sums, assignment.reshape(NZ, LANES))


def grads_kernel(inner_ref, own_ref, other_ref, scale_ref, out_ref, acc):
    acc[...] = jnp.zeros_like(acc)
    tiles = 4
    span = tiles * LANES
    query = lax.broadcasted_iota(jnp.int32, (QUERIES, span), 0).astype(f32)

    def row(r, carry):
        owners = own_ref[r, OWNER_ROW:, :].astype(f32)
        for p in range(NZ // tiles):
            inner = inner_ref[r, :, p * span : (p + 1) * span].astype(f32)
            cut = range(p * tiles, (p + 1) * tiles)
            parts = []
            for ref in (own_ref, other_ref):
                outer = jnp.concatenate([ref[r, t * NI : (t + 1) * NI, :] for t in cut], axis=1).astype(f32)
                parts.append((outer[:, None, :] * inner[None, :, :]).reshape(HALF, span).astype(bf16))
            product = jnp.concatenate(parts, axis=0)
            owner = jnp.concatenate([owners[t : t + 1, :] for t in cut], axis=1)
            mine = jnp.where(query == owner, 1.0, 0.0).astype(bf16)
            acc[...] += lax.dot_general(product, mine, (((1,), (1,)), ((), ())), preferred_element_type=f32)
        return carry

    lax.fori_loop(0, NZ, row, 0)
    out_ref[...] = (acc[...].T * scale_ref[...]).astype(bf16)


def query_grads(inner, own, other, scale):
    return pl.pallas_call(
        grads_kernel,
        in_specs=[VMEM] * 4,
        out_specs=VMEM,
        out_shape=jax.ShapeDtypeStruct((QUERIES, 2 * HALF), bf16),
        scratch_shapes=[pltpu.VMEM((2 * HALF, QUERIES), f32)],
        compiler_params=SMALL,
        name="query_grads",
    )(inner, own, other, scale)


def share_kernel(terms_ref, out_ref):
    total = terms_ref[0].astype(f32)
    for y in range(1, NY):
        total += terms_ref[y].astype(f32)
    share = total.astype(bf16)
    for y in range(NY * ZH):
        out_ref[y] = share


def spread_share(terms):
    return pl.pallas_call(
        share_kernel,
        in_specs=[VMEM],
        out_specs=VMEM,
        out_shape=jax.ShapeDtypeStruct((NY * ZH, *terms.shape[1:]), bf16),
        compiler_params=SMALL,
        name="spread_share",
    )(terms)


def terms_kernel(place_ref, scaled_ref, other_ref, *refs):
    own, (keep_ref, send_ref) = refs[:ZL], refs[ZL:]
    zl, c = place_ref[0], place_ref[1]
    for k in range(ZL):
        terms = jnp.zeros((QUERIES, other_ref.shape[3]), f32)
        for h in range(ZH):
            terms += jnp.dot(scaled_ref[h, :, :HALF], own[k][0, h], preferred_element_type=f32)
            terms += jnp.dot(scaled_ref[h, :, HALF:], other_ref[k, h], preferred_element_type=f32)
        terms = terms.reshape(NW, 2, QUERIES // NF, terms.shape[1])
        first, second = terms[:, 0], terms[:, 1]
        keep_ref[:, zl ^ k] = jnp.where(c == 0, first, second)
        send_ref[:, zl ^ k] = jnp.where(c == 0, second, first)


def score_terms(place, scaled, own, other):
    shape = jax.ShapeDtypeStruct((NW, ZL, QUERIES // NF, other.shape[3]), f32)
    return pl.pallas_call(
        terms_kernel,
        in_specs=[SMEM] + [VMEM] * (2 + ZL),
        out_specs=[VMEM] * 2,
        out_shape=[shape, shape],
        compiler_params=SMALL,
        name="score_terms",
    )(place, scaled, other, *own)


def late_kernel(place_ref, out_ref):
    for i in range(out_ref.shape[0]):
        out_ref[i] = place_ref[i]


def late_place(place):
    return pl.pallas_call(
        late_kernel,
        in_specs=[SMEM],
        out_specs=SMEM,
        out_shape=jax.ShapeDtypeStruct(place.shape, place.dtype),
        name="late_place",
    )(place)


def local(acts, out_grads, proj_in, proj_out, assignment, codes, zero_points, scales):
    zl = lax.axis_index("zl")
    z = zl * ZH + lax.axis_index("zh")
    c = lax.axis_index("c")
    place = jnp.stack([zl, c, z]).astype(jnp.int32)
    flip = [(0, 1), (1, 0)]

    keep, send = project(place, acts, out_grads, proj_in, proj_out)
    got = lax.ppermute(send, "c", flip)
    parts = ((keep + got) * LINK_GAIN).astype(f16)
    parts = exchange(parts, ("yl", "x"))
    sums = jnp.sum(parts.astype(f32), axis=0)

    inner, packed = pack_tokens(sums, assignment)
    own = exchange(packed, ("zl", "zh"))
    swap = [(r * NW + w, w * NW + r) for r in range(NZ) for w in range(NW)]
    inner = lax.ppermute(inner, ("zl", "zh", "yl", "x"), swap)
    inner = exchange(jnp.broadcast_to(inner[None], (NW, *inner.shape)), ("yl", "x"))
    other = lax.ppermute(own, "c", flip)

    store = list(store_levels(place, codes, zero_points))
    for k in range(1, ZL):
        store[k] = lax.ppermute(store[k], "zl", [(r, r ^ k) for r in range(ZL)])
    store_other = lax.ppermute(jnp.stack([block[1] for block in store]), "c", flip)

    own_scale, other_scale = pick_scales(place, scales)
    other_scale = lax.ppermute(other_scale, "c", flip)
    scale = jnp.concatenate([own_scale, other_scale], axis=0).reshape(1, 2 * HALF)

    grads = query_grads(inner, own, other, scale)
    grads = exchange(grads.reshape(NY, QUERIES // NY, 2 * HALF), "yh")
    place = late_place(place)
    scaled = exchange(spread_share(grads), ("zh", "yh")).reshape(ZH, QUERIES, 2 * HALF)

    keep, send = score_terms(place, scaled, store, store_other)
    got = lax.ppermute(send, "c", flip)
    terms = exchange((keep + got).astype(bf16), ("yl", "x"))
    terms = exchange(jnp.sum(terms.astype(f32), axis=0), "zl")
    return jnp.sum(terms.reshape(ZL, QUERIES // NF, codes.shape[0]), axis=0)


def solution(mesh):
    split = Mesh(mesh.devices.reshape(4, 4, 2, 2, 4, 2), AXES)
    in_specs = (
        P(ROWS, FEAT),
        P(ROWS, FEAT),
        P(FEAT, None),
        P(FEAT, None),
        P(ROWS),
        P(ROWS, FEAT),
        P(FEAT),
        P(FEAT),
    )
    out_specs = P(FEAT, ROWS)
    return jax.shard_map(local, mesh=split, in_specs=in_specs, out_specs=out_specs, check_vma=False)
```

```python
import jax
import jax.numpy as jnp
from jax import lax
from jax.experimental import pallas as pl
from jax.experimental.pallas import tpu as pltpu
from jax.sharding import Mesh
from jax.sharding import PartitionSpec as P


RANK = 256
QUERIES = 256
AXES = ("yh", "zl", "zh", "yl", "x", "c")
ROWS = ("yh", "zl", "zh")
FEAT = ("yl", "x", "c")
NY = 4
NZ = 8
ZH = 2
ZL = 4
NW = 8
NF = 16
NI = 16
NJ = 16
HALF = NI * NJ
LANES = 128
OWNER_ROW = 128
PACKED_ROWS = 144
LINK_GAIN = 128.0
f32 = jnp.float32
bf16 = jnp.bfloat16
f16 = jnp.float16
VMEM = pl.BlockSpec(memory_space=pltpu.VMEM)
SMEM = pl.BlockSpec(memory_space=pltpu.SMEM)
SMALL = pltpu.CompilerParams(vmem_limit_bytes=16 * 2**20)


def exchange(blocks, axes):
    return lax.all_to_all(blocks, axes, 0, 0, tiled=True)


def store_kernel(codes_ref, zero_ref, *refs):
    outs, turned = refs[:ZL], refs[ZL]
    zl, c = lax.axis_index("zl"), lax.axis_index("c")
    for i in range(codes_ref.shape[1] // RANK):
        cols = slice(i * RANK, (i + 1) * RANK)
        turned[...] = (codes_ref[:, cols] - zero_ref[:, cols]).astype(f32).T
        for k in range(ZL):
            for s in range(2):
                for h in range(ZH):
                    block = (c ^ s) * NZ + (zl ^ k) * ZH + h
                    rows = pl.ds(pl.multiple_of(block * NJ, NJ), NJ)
                    outs[k][s, h, i * NJ : (i + 1) * NJ, :] = turned[rows, :].astype(bf16)


def store_levels(codes, zero_points):
    rows = codes.shape[0]
    step = 4
    return pl.pallas_call(
        store_kernel,
        grid=(NI // step,),
        in_specs=[
            pl.BlockSpec((rows, step * RANK), lambda g: (0, g)),
            pl.BlockSpec((1, step * RANK), lambda g: (0, g)),
        ],
        out_specs=[pl.BlockSpec((2, ZH, step * NJ, rows), lambda g: (0, 0, g, 0))] * ZL,
        out_shape=[jax.ShapeDtypeStruct((2, ZH, HALF, rows), bf16)] * ZL,
        scratch_shapes=[pltpu.VMEM((RANK, rows), f32)],
        compiler_params=SMALL,
        name="store_levels",
    )(codes, zero_points.reshape(1, -1))


def pick_kernel(scales_ref, own_ref, other_ref):
    c, z = lax.axis_index("c"), lax.axis_index(("zl", "zh"))
    own_ref[...] = scales_ref[:, pl.ds(c * NZ + z, 1), :]
    other_ref[...] = scales_ref[:, pl.ds((1 - c) * NZ + z, 1), :]


def pick_scales(scales):
    return pl.pallas_call(
        pick_kernel,
        in_specs=[VMEM],
        out_specs=[VMEM] * 2,
        out_shape=[jax.ShapeDtypeStruct((NI, 1, NJ), f32)] * 2,
        compiler_params=SMALL,
        name="pick_scales",
    )(scales.reshape(NI, NF, NJ))


def project_kernel(acts_ref, grads_ref, in_ref, out_ref, keep_ref, send_ref, turned, full):
    c = lax.axis_index("c")

    @pl.when(pl.program_id(0) == 0)
    def turn():
        turned[0] = in_ref[...].T
        turned[1] = out_ref[...].T

    for side, ref in enumerate((acts_ref, grads_ref)):
        full[side] = lax.dot_general(
            turned[side], ref[...], (((1,), (1,)), ((), ())), preferred_element_type=f32
        )
    for w in range(NW):
        for ref, core in ((keep_ref, c), (send_ref, 1 - c)):
            rows = pl.ds(pl.multiple_of((core * NZ + w) * NJ, NJ), NJ)
            ref[w, :NJ, :] = full[0, rows, :]
            rows = pl.ds(pl.multiple_of((w * 2 + core) * NI, NI), NI)
            ref[w, NJ:, :] = full[1, rows, :]


def project(acts, out_grads, proj_in, proj_out):
    tokens, depth = acts.shape
    span = 2 * LANES
    wide = pl.BlockSpec((span, depth), lambda g: (g, 0))
    whole = pl.BlockSpec((depth, RANK), lambda g: (0, 0))
    shape = jax.ShapeDtypeStruct((NW, NJ + NI, tokens), f32)
    return pl.pallas_call(
        project_kernel,
        grid=(tokens // span,),
        in_specs=[wide, wide, whole, whole],
        out_specs=[pl.BlockSpec((NW, NJ + NI, span), lambda g: (0, 0, g))] * 2,
        out_shape=[shape] * 2,
        scratch_shapes=[pltpu.VMEM((2, RANK, depth), bf16), pltpu.VMEM((2, RANK, span), f32)],
        name="project",
    )(acts, out_grads, proj_in, proj_out)


def pack_kernel(sums_ref, owner_ref, inner_ref, packed_ref):
    values = sums_ref[...] * (1.0 / LINK_GAIN)
    inner_ref[...] = values[:NJ].astype(bf16)
    outer = values[NJ:].astype(bf16)
    owners = owner_ref[...].astype(f32)
    tail = jnp.concatenate([owners, jnp.zeros_like(owners)], axis=0).astype(bf16)
    for r in range(NZ):
        for t in range(NZ):
            packed_ref[r, t * NI : (t + 1) * NI, :] = outer[:, t * LANES : (t + 1) * LANES]
        packed_ref[r, OWNER_ROW:, :] = tail


def pack_tokens(sums, assignment):
    return pl.pallas_call(
        pack_kernel,
        in_specs=[VMEM] * 2,
        out_specs=[VMEM] * 2,
        out_shape=[
            jax.ShapeDtypeStruct((NJ, sums.shape[1]), bf16),
            jax.ShapeDtypeStruct((NZ, PACKED_ROWS, LANES), bf16),
        ],
        compiler_params=SMALL,
        name="pack_tokens",
    )(sums, assignment.reshape(NZ, LANES))


def grads_kernel(inner_ref, own_ref, other_ref, scale_ref, out_ref, acc):
    acc[...] = jnp.zeros_like(acc)
    tiles = 4
    span = tiles * LANES
    query = lax.broadcasted_iota(jnp.int32, (QUERIES, span), 0).astype(f32)

    def row(r, carry):
        owners = own_ref[r, OWNER_ROW:, :].astype(f32)
        for p in range(NZ // tiles):
            inner = inner_ref[r, :, p * span : (p + 1) * span].astype(f32)
            cut = range(p * tiles, (p + 1) * tiles)
            parts = []
            for ref in (own_ref, other_ref):
                outer = jnp.concatenate([ref[r, t * NI : (t + 1) * NI, :] for t in cut], axis=1).astype(f32)
                parts.append((outer[:, None, :] * inner[None, :, :]).reshape(HALF, span).astype(bf16))
            product = jnp.concatenate(parts, axis=0)
            owner = jnp.concatenate([owners[t : t + 1, :] for t in cut], axis=1)
            mine = jnp.where(query == owner, 1.0, 0.0).astype(bf16)
            acc[...] += lax.dot_general(product, mine, (((1,), (1,)), ((), ())), preferred_element_type=f32)
        return carry

    lax.fori_loop(0, NZ, row, 0, unroll=4)
    out_ref[...] = (acc[...].T * scale_ref[...]).astype(bf16)


def query_grads(inner, own, other, scale):
    return pl.pallas_call(
        grads_kernel,
        in_specs=[VMEM] * 4,
        out_specs=VMEM,
        out_shape=jax.ShapeDtypeStruct((QUERIES, 2 * HALF), bf16),
        scratch_shapes=[pltpu.VMEM((2 * HALF, QUERIES), f32)],
        compiler_params=SMALL,
        name="query_grads",
    )(inner, own, other, scale)


def share_kernel(terms_ref, out_ref):
    total = terms_ref[0].astype(f32)
    for y in range(1, NY):
        total += terms_ref[y].astype(f32)
    share = total.astype(bf16)
    for y in range(NY * ZH):
        out_ref[y] = share


def spread_share(terms):
    return pl.pallas_call(
        share_kernel,
        in_specs=[VMEM],
        out_specs=VMEM,
        out_shape=jax.ShapeDtypeStruct((NY * ZH, *terms.shape[1:]), bf16),
        compiler_params=SMALL,
        name="spread_share",
    )(terms)


def terms_kernel(late_ref, scaled_ref, other_ref, *refs):
    own, (keep_ref, send_ref) = refs[:ZL], refs[ZL:]
    zl, c = late_ref[0], lax.axis_index("c")
    for k in range(ZL):
        terms = jnp.zeros((QUERIES, other_ref.shape[3]), f32)
        for h in range(ZH):
            terms += jnp.dot(scaled_ref[h, :, :HALF], own[k][0, h], preferred_element_type=f32)
            terms += jnp.dot(scaled_ref[h, :, HALF:], other_ref[k, h], preferred_element_type=f32)
        terms = terms.reshape(NW, 2, QUERIES // NF, terms.shape[1])
        first, second = terms[:, 0], terms[:, 1]
        keep_ref[zl ^ k] = jnp.where(c == 0, first, second)
        send_ref[zl ^ k] = jnp.where(c == 0, second, first)


def score_terms(late, scaled, own, other):
    shape = jax.ShapeDtypeStruct((ZL, NW, QUERIES // NF, other.shape[3]), f32)
    return pl.pallas_call(
        terms_kernel,
        in_specs=[SMEM] + [VMEM] * (2 + ZL),
        out_specs=[VMEM] * 2,
        out_shape=[shape, shape],
        compiler_params=SMALL,
        name="score_terms",
    )(late, scaled, other, *own)


def late_kernel(place_ref, out_ref):
    for i in range(out_ref.shape[0]):
        out_ref[i] = place_ref[i]


def late_place(place):
    return pl.pallas_call(
        late_kernel,
        in_specs=[SMEM],
        out_specs=SMEM,
        out_shape=jax.ShapeDtypeStruct(place.shape, place.dtype),
        name="late_place",
    )(place)


def local(acts, out_grads, proj_in, proj_out, assignment, codes, zero_points, scales):
    flip = [(0, 1), (1, 0)]
    keep, send = project(acts, out_grads, proj_in, proj_out)
    got = lax.ppermute(send, "c", flip)
    parts = ((keep + got) * LINK_GAIN).astype(f16)
    parts = exchange(parts, ("yl", "x"))
    sums = jnp.sum(parts.astype(f32), axis=0)

    inner, packed = pack_tokens(sums, assignment)
    own = exchange(packed, ("zl", "zh"))
    swap = [(r * NW + w, w * NW + r) for r in range(NZ) for w in range(NW)]
    inner = lax.ppermute(inner, ("zl", "zh", "yl", "x"), swap)
    inner = exchange(jnp.broadcast_to(inner[None], (NW, *inner.shape)), ("yl", "x"))
    other = lax.ppermute(own, "c", flip)

    store = list(store_levels(codes, zero_points))
    for k in range(1, ZL):
        store[k] = lax.ppermute(store[k], "zl", [(r, r ^ k) for r in range(ZL)])
    store_other = lax.ppermute(jnp.stack([block[1] for block in store]), "c", flip)

    own_scale, other_scale = pick_scales(scales)
    other_scale = lax.ppermute(other_scale, "c", flip)
    scale = jnp.concatenate([own_scale, other_scale], axis=0).reshape(1, 2 * HALF)

    late = late_place(lax.axis_index("zl").reshape(1).astype(jnp.int32))
    grads = query_grads(inner, own, other, scale)
    grads = exchange(grads.reshape(NY, QUERIES // NY, 2 * HALF), "yh")
    scaled = exchange(spread_share(grads), ("zh", "yh")).reshape(ZH, QUERIES, 2 * HALF)

    keep, send = score_terms(late, scaled, store, store_other)
    got = lax.ppermute(send, "c", flip)
    terms = (keep + got).astype(bf16).reshape(ZL * NW, QUERIES // NF, codes.shape[0])
    terms = exchange(terms, ("zl", "yl", "x"))
    return jnp.sum(terms.astype(f32), axis=0)


def solution(mesh):
    split = Mesh(mesh.devices.reshape(4, 4, 2, 2, 4, 2), AXES)
    in_specs = (
        P(ROWS, FEAT),
        P(ROWS, FEAT),
        P(FEAT, None),
        P(FEAT, None),
        P(ROWS),
        P(ROWS, FEAT),
        P(FEAT),
        P(FEAT),
    )
    out_specs = P(FEAT, ROWS)
    return jax.shard_map(local, mesh=split, in_specs=in_specs, out_specs=out_specs, check_vma=False)
```

```python
import jax
import jax.numpy as jnp
from jax import lax
from jax.experimental import pallas as pl
from jax.experimental.pallas import tpu as pltpu
from jax.sharding import Mesh
from jax.sharding import PartitionSpec as P


RANK = 256
QUERIES = 256
AXES = ("yh", "zl", "zh", "yl", "x", "c")
ROWS = ("yh", "zl", "zh")
FEAT = ("yl", "x", "c")
NY = 4
NZ = 8
ZH = 2
ZL = 4
NW = 8
NF = 16
NI = 16
NJ = 16
HALF = NI * NJ
LANES = 128
OWNER_ROW = 128
PACKED_ROWS = 144
LINK_GAIN = 128.0
f32 = jnp.float32
bf16 = jnp.bfloat16
f16 = jnp.float16
VMEM = pl.BlockSpec(memory_space=pltpu.VMEM)
SMEM = pl.BlockSpec(memory_space=pltpu.SMEM)
SMALL = pltpu.CompilerParams(vmem_limit_bytes=16 * 2**20)


def exchange(blocks, axes):
    return lax.all_to_all(blocks, axes, 0, 0, tiled=True)


def store_kernel(codes_ref, zero_ref, *refs):
    outs, turned = refs[:ZL], refs[ZL]
    zl, c = lax.axis_index("zl"), lax.axis_index("c")
    for i in range(codes_ref.shape[1] // RANK):
        cols = slice(i * RANK, (i + 1) * RANK)
        turned[...] = (codes_ref[:, cols] - zero_ref[:, cols]).astype(f32).T
        for k in range(ZL):
            for s in range(2):
                for h in range(ZH):
                    block = (c ^ s) * NZ + (zl ^ k) * ZH + h
                    rows = pl.ds(pl.multiple_of(block * NJ, NJ), NJ)
                    outs[k][s, h, i * NJ : (i + 1) * NJ, :] = turned[rows, :].astype(bf16)


def store_levels(codes, zero_points):
    rows = codes.shape[0]
    step = 4
    return pl.pallas_call(
        store_kernel,
        grid=(NI // step,),
        in_specs=[
            pl.BlockSpec((rows, step * RANK), lambda g: (0, g)),
            pl.BlockSpec((1, step * RANK), lambda g: (0, g)),
        ],
        out_specs=[pl.BlockSpec((2, ZH, step * NJ, rows), lambda g: (0, 0, g, 0))] * ZL,
        out_shape=[jax.ShapeDtypeStruct((2, ZH, HALF, rows), bf16)] * ZL,
        scratch_shapes=[pltpu.VMEM((RANK, rows), f32)],
        compiler_params=SMALL,
        name="store_levels",
    )(codes, zero_points.reshape(1, -1))


def pick_kernel(scales_ref, own_ref, other_ref):
    c, z = lax.axis_index("c"), lax.axis_index(("zl", "zh"))
    own_ref[...] = scales_ref[:, pl.ds(c * NZ + z, 1), :]
    other_ref[...] = scales_ref[:, pl.ds((1 - c) * NZ + z, 1), :]


def pick_scales(scales):
    return pl.pallas_call(
        pick_kernel,
        in_specs=[VMEM],
        out_specs=[VMEM] * 2,
        out_shape=[jax.ShapeDtypeStruct((NI, 1, NJ), f32)] * 2,
        compiler_params=SMALL,
        name="pick_scales",
    )(scales.reshape(NI, NF, NJ))


def project_kernel(acts_ref, grads_ref, in_ref, out_ref, keep_ref, send_ref, full):
    c = lax.axis_index("c")
    for side, (rows_ref, proj_ref) in enumerate(((acts_ref, in_ref), (grads_ref, out_ref))):
        full[side] = jnp.dot(rows_ref[...], proj_ref[...], preferred_element_type=f32).T
    for w in range(NW):
        for ref, core in ((keep_ref, c), (send_ref, 1 - c)):
            rows = pl.ds(pl.multiple_of((core * NZ + w) * NJ, NJ), NJ)
            ref[w, :NJ, :] = full[0, rows, :]
            rows = pl.ds(pl.multiple_of((w * 2 + core) * NI, NI), NI)
            ref[w, NJ:, :] = full[1, rows, :]


def project(acts, out_grads, proj_in, proj_out):
    tokens, depth = acts.shape
    span = 4 * LANES
    wide = pl.BlockSpec((span, depth), lambda g: (g, 0))
    whole = pl.BlockSpec((depth, RANK), lambda g: (0, 0))
    shape = jax.ShapeDtypeStruct((NW, NJ + NI, tokens), f32)
    return pl.pallas_call(
        project_kernel,
        grid=(tokens // span,),
        in_specs=[wide, wide, whole, whole],
        out_specs=[pl.BlockSpec((NW, NJ + NI, span), lambda g: (0, 0, g))] * 2,
        out_shape=[shape] * 2,
        scratch_shapes=[pltpu.VMEM((2, RANK, span), f32)],
        name="project",
    )(acts, out_grads, proj_in, proj_out)


def pack_kernel(sums_ref, owner_ref, inner_ref, packed_ref):
    values = sums_ref[...] * (1.0 / LINK_GAIN)
    inner_ref[...] = values[:NJ].astype(bf16)
    outer = values[NJ:].astype(bf16)
    owners = owner_ref[...].astype(f32)
    tail = jnp.concatenate([owners, jnp.zeros_like(owners)], axis=0).astype(bf16)
    for r in range(NZ):
        for t in range(NZ):
            packed_ref[r, t * NI : (t + 1) * NI, :] = outer[:, t * LANES : (t + 1) * LANES]
        packed_ref[r, OWNER_ROW:, :] = tail


def pack_tokens(sums, assignment):
    return pl.pallas_call(
        pack_kernel,
        in_specs=[VMEM] * 2,
        out_specs=[VMEM] * 2,
        out_shape=[
            jax.ShapeDtypeStruct((NJ, sums.shape[1]), bf16),
            jax.ShapeDtypeStruct((NZ, PACKED_ROWS, LANES), bf16),
        ],
        compiler_params=SMALL,
        name="pack_tokens",
    )(sums, assignment.reshape(NZ, LANES))


def grads_kernel(inner_ref, own_ref, other_ref, scale_ref, out_ref, acc):
    acc[...] = jnp.zeros_like(acc)
    tiles = 4
    span = tiles * LANES
    query = lax.broadcasted_iota(jnp.int32, (QUERIES, span), 0).astype(f32)

    def row(r, carry):
        owners = own_ref[r, OWNER_ROW:, :].astype(f32)
        for p in range(NZ // tiles):
            inner = inner_ref[r, :, p * span : (p + 1) * span].astype(f32)
            cut = range(p * tiles, (p + 1) * tiles)
            parts = []
            for ref in (own_ref, other_ref):
                outer = jnp.concatenate([ref[r, t * NI : (t + 1) * NI, :] for t in cut], axis=1).astype(f32)
                parts.append((outer[:, None, :] * inner[None, :, :]).reshape(HALF, span).astype(bf16))
            product = jnp.concatenate(parts, axis=0)
            owner = jnp.concatenate([owners[t : t + 1, :] for t in cut], axis=1)
            mine = jnp.where(query == owner, 1.0, 0.0).astype(bf16)
            acc[...] += lax.dot_general(product, mine, (((1,), (1,)), ((), ())), preferred_element_type=f32)
        return carry

    lax.fori_loop(0, NZ, row, 0, unroll=4)
    out_ref[...] = (acc[...].T * scale_ref[...]).astype(bf16)


def query_grads(inner, own, other, scale):
    return pl.pallas_call(
        grads_kernel,
        in_specs=[VMEM] * 4,
        out_specs=VMEM,
        out_shape=jax.ShapeDtypeStruct((QUERIES, 2 * HALF), bf16),
        scratch_shapes=[pltpu.VMEM((2 * HALF, QUERIES), f32)],
        compiler_params=SMALL,
        name="query_grads",
    )(inner, own, other, scale)


def share_kernel(terms_ref, out_ref):
    total = terms_ref[0].astype(f32)
    for y in range(1, NY):
        total += terms_ref[y].astype(f32)
    share = total.astype(bf16)
    for y in range(NY * ZH):
        out_ref[y] = share


def spread_share(terms):
    return pl.pallas_call(
        share_kernel,
        in_specs=[VMEM],
        out_specs=VMEM,
        out_shape=jax.ShapeDtypeStruct((NY * ZH, *terms.shape[1:]), bf16),
        compiler_params=SMALL,
        name="spread_share",
    )(terms)


def terms_kernel(late_ref, scaled_ref, other_ref, *refs):
    own, (keep_ref, send_ref) = refs[:ZL], refs[ZL:]
    zl, c = late_ref[0], lax.axis_index("c")
    for k in range(ZL):
        terms = jnp.zeros((QUERIES, other_ref.shape[3]), f32)
        for h in range(ZH):
            terms += jnp.dot(scaled_ref[h, :, :HALF], own[k][0, h], preferred_element_type=f32)
            terms += jnp.dot(scaled_ref[h, :, HALF:], other_ref[k, h], preferred_element_type=f32)
        terms = terms.reshape(NW, 2, QUERIES // NF, terms.shape[1])
        first, second = terms[:, 0], terms[:, 1]
        keep_ref[zl ^ k] = jnp.where(c == 0, first, second)
        send_ref[zl ^ k] = jnp.where(c == 0, second, first)


def score_terms(late, scaled, own, other):
    shape = jax.ShapeDtypeStruct((ZL, NW, QUERIES // NF, other.shape[3]), f32)
    return pl.pallas_call(
        terms_kernel,
        in_specs=[SMEM] + [VMEM] * (2 + ZL),
        out_specs=[VMEM] * 2,
        out_shape=[shape, shape],
        compiler_params=SMALL,
        name="score_terms",
    )(late, scaled, other, *own)


def late_kernel(place_ref, out_ref):
    for i in range(out_ref.shape[0]):
        out_ref[i] = place_ref[i]


def late_place(place):
    return pl.pallas_call(
        late_kernel,
        in_specs=[SMEM],
        out_specs=SMEM,
        out_shape=jax.ShapeDtypeStruct(place.shape, place.dtype),
        name="late_place",
    )(place)


def local(acts, out_grads, proj_in, proj_out, assignment, codes, zero_points, scales):
    flip = [(0, 1), (1, 0)]
    keep, send = project(acts, out_grads, proj_in, proj_out)
    got = lax.ppermute(send, "c", flip)
    parts = ((keep + got) * LINK_GAIN).astype(f16)
    parts = exchange(parts, ("yl", "x"))
    sums = jnp.sum(parts.astype(f32), axis=0)

    inner, packed = pack_tokens(sums, assignment)
    own = exchange(packed, ("zl", "zh"))
    swap = [(r * NW + w, w * NW + r) for r in range(NZ) for w in range(NW)]
    inner = lax.ppermute(inner, ("zl", "zh", "yl", "x"), swap)
    inner = exchange(jnp.broadcast_to(inner[None], (NW, *inner.shape)), ("yl", "x"))
    other = lax.ppermute(own, "c", flip)

    store = list(store_levels(codes, zero_points))
    for k in range(1, ZL):
        store[k] = lax.ppermute(store[k], "zl", [(r, r ^ k) for r in range(ZL)])
    store_other = lax.ppermute(jnp.stack([block[1] for block in store]), "c", flip)

    own_scale, other_scale = pick_scales(scales)
    other_scale = lax.ppermute(other_scale, "c", flip)
    scale = jnp.concatenate([own_scale, other_scale], axis=0).reshape(1, 2 * HALF)

    late = late_place(lax.axis_index("zl").reshape(1).astype(jnp.int32))
    grads = query_grads(inner, own, other, scale)
    grads = exchange(grads.reshape(NY, QUERIES // NY, 2 * HALF), "yh")
    scaled = exchange(spread_share(grads), ("zh", "yh")).reshape(ZH, QUERIES, 2 * HALF)

    keep, send = score_terms(late, scaled, store, store_other)
    got = lax.ppermute(send, "c", flip)
    terms = (keep + got).astype(bf16).reshape(ZL * NW, QUERIES // NF, codes.shape[0])
    terms = exchange(terms, ("zl", "yl", "x"))
    return jnp.sum(terms.astype(f32), axis=0)


def solution(mesh):
    split = Mesh(mesh.devices.reshape(4, 4, 2, 2, 4, 2), AXES)
    in_specs = (
        P(ROWS, FEAT),
        P(ROWS, FEAT),
        P(FEAT, None),
        P(FEAT, None),
        P(ROWS),
        P(ROWS, FEAT),
        P(FEAT),
        P(FEAT),
    )
    out_specs = P(FEAT, ROWS)
    return jax.shard_map(local, mesh=split, in_specs=in_specs, out_specs=out_specs, check_vma=False)
```

```python
import jax
import jax.numpy as jnp
from jax import lax
from jax.experimental import pallas as pl
from jax.experimental.pallas import tpu as pltpu
from jax.sharding import Mesh
from jax.sharding import PartitionSpec as P


RANK = 256
QUERIES = 256
AXES = ("yh", "zl", "zh", "yl", "x", "c")
ROWS = ("yh", "zl", "zh")
FEAT = ("yl", "x", "c")
NY = 4
NZ = 8
ZH = 2
ZL = 4
NW = 8
NF = 16
NI = 16
NJ = 16
HALF = NI * NJ
LANES = 128
OWNER_ROW = 128
PACKED_ROWS = 136
LINK_GAIN = 128.0
f32 = jnp.float32
bf16 = jnp.bfloat16
f16 = jnp.float16
VMEM = pl.BlockSpec(memory_space=pltpu.VMEM)
SMEM = pl.BlockSpec(memory_space=pltpu.SMEM)
SMALL = pltpu.CompilerParams(vmem_limit_bytes=16 * 2**20)


def exchange(blocks, axes):
    return lax.all_to_all(blocks, axes, 0, 0, tiled=True)


def store_kernel(codes_ref, zero_ref, *refs):
    outs, turned = refs[:ZL], refs[ZL]
    zl, c = lax.axis_index("zl"), lax.axis_index("c")
    for i in range(codes_ref.shape[1] // RANK):
        cols = slice(i * RANK, (i + 1) * RANK)
        turned[...] = (codes_ref[:, cols] - zero_ref[:, cols]).astype(f32).T
        for k in range(ZL):
            for s in range(2):
                for h in range(ZH):
                    block = (c ^ s) * NZ + (zl ^ k) * ZH + h
                    rows = pl.ds(pl.multiple_of(block * NJ, NJ), NJ)
                    outs[k][s, h, i * NJ : (i + 1) * NJ, :] = turned[rows, :].astype(bf16)


def store_levels(codes, zero_points):
    rows = codes.shape[0]
    step = 4
    return pl.pallas_call(
        store_kernel,
        grid=(NI // step,),
        in_specs=[
            pl.BlockSpec((rows, step * RANK), lambda g: (0, g)),
            pl.BlockSpec((1, step * RANK), lambda g: (0, g)),
        ],
        out_specs=[pl.BlockSpec((2, ZH, step * NJ, rows), lambda g: (0, 0, g, 0))] * ZL,
        out_shape=[jax.ShapeDtypeStruct((2, ZH, HALF, rows), bf16)] * ZL,
        scratch_shapes=[pltpu.VMEM((RANK, rows), f32)],
        compiler_params=SMALL,
        name="store_levels",
    )(codes, zero_points.reshape(1, -1))


def pick_kernel(scales_ref, own_ref, other_ref):
    c, z = lax.axis_index("c"), lax.axis_index(("zl", "zh"))
    own_ref[...] = scales_ref[:, pl.ds(c * NZ + z, 1), :]
    other_ref[...] = scales_ref[:, pl.ds((1 - c) * NZ + z, 1), :]


def pick_scales(scales):
    return pl.pallas_call(
        pick_kernel,
        in_specs=[VMEM],
        out_specs=[VMEM] * 2,
        out_shape=[jax.ShapeDtypeStruct((NI, 1, NJ), f32)] * 2,
        compiler_params=SMALL,
        name="pick_scales",
    )(scales.reshape(NI, NF, NJ))


def project_kernel(acts_ref, grads_ref, in_ref, out_ref, keep_ref, send_ref, full):
    c = lax.axis_index("c")
    for side, (rows_ref, proj_ref) in enumerate(((acts_ref, in_ref), (grads_ref, out_ref))):
        full[side] = jnp.dot(rows_ref[...], proj_ref[...], preferred_element_type=f32).T
    for w in range(NW):
        for ref, core in ((keep_ref, c), (send_ref, 1 - c)):
            rows = pl.ds(pl.multiple_of((core * NZ + w) * NJ, NJ), NJ)
            ref[w, :NJ, :] = full[0, rows, :]
            rows = pl.ds(pl.multiple_of((w * 2 + core) * NI, NI), NI)
            ref[w, NJ:, :] = full[1, rows, :]


def project(acts, out_grads, proj_in, proj_out):
    tokens, depth = acts.shape
    span = 4 * LANES
    wide = pl.BlockSpec((span, depth), lambda g: (g, 0))
    whole = pl.BlockSpec((depth, RANK), lambda g: (0, 0))
    shape = jax.ShapeDtypeStruct((NW, NJ + NI, tokens), f32)
    return pl.pallas_call(
        project_kernel,
        grid=(tokens // span,),
        in_specs=[wide, wide, whole, whole],
        out_specs=[pl.BlockSpec((NW, NJ + NI, span), lambda g: (0, 0, g))] * 2,
        out_shape=[shape] * 2,
        scratch_shapes=[pltpu.VMEM((2, RANK, span), f32)],
        name="project",
    )(acts, out_grads, proj_in, proj_out)


def pack_kernel(sums_ref, owner_ref, inner_ref, packed_ref):
    values = sums_ref[...] * (1.0 / LINK_GAIN)
    inner_ref[...] = values[:NJ].astype(bf16)
    outer = values[NJ:].astype(bf16)
    owners = owner_ref[...].astype(f32)
    tail = owners.astype(bf16)
    for r in range(NZ):
        for t in range(NZ):
            packed_ref[r, t * NI : (t + 1) * NI, :] = outer[:, t * LANES : (t + 1) * LANES]
        packed_ref[r, OWNER_ROW:, :] = tail


def pack_tokens(sums, assignment):
    return pl.pallas_call(
        pack_kernel,
        in_specs=[VMEM] * 2,
        out_specs=[VMEM] * 2,
        out_shape=[
            jax.ShapeDtypeStruct((NJ, sums.shape[1]), bf16),
            jax.ShapeDtypeStruct((NZ, PACKED_ROWS, LANES), bf16),
        ],
        compiler_params=SMALL,
        name="pack_tokens",
    )(sums, assignment.reshape(NZ, LANES))


def grads_kernel(inner_ref, own_ref, other_ref, scale_ref, out_ref, acc):
    acc[...] = jnp.zeros_like(acc)
    tiles = 4
    span = tiles * LANES
    query = lax.broadcasted_iota(jnp.int32, (QUERIES, span), 0).astype(f32)

    def row(r, carry):
        owners = own_ref[r, OWNER_ROW:, :].astype(f32)
        for p in range(NZ // tiles):
            inner = inner_ref[r, :, p * span : (p + 1) * span].astype(f32)
            cut = range(p * tiles, (p + 1) * tiles)
            parts = []
            for ref in (own_ref, other_ref):
                outer = jnp.concatenate([ref[r, t * NI : (t + 1) * NI, :] for t in cut], axis=1).astype(f32)
                parts.append((outer[:, None, :] * inner[None, :, :]).reshape(HALF, span).astype(bf16))
            product = jnp.concatenate(parts, axis=0)
            owner = jnp.concatenate([owners[t : t + 1, :] for t in cut], axis=1)
            mine = jnp.where(query == owner, 1.0, 0.0).astype(bf16)
            acc[...] += lax.dot_general(product, mine, (((1,), (1,)), ((), ())), preferred_element_type=f32)
        return carry

    lax.fori_loop(0, NZ, row, 0, unroll=8)
    out_ref[...] = (acc[...].T * scale_ref[...]).astype(bf16)


def query_grads(inner, own, other, scale):
    return pl.pallas_call(
        grads_kernel,
        in_specs=[VMEM] * 4,
        out_specs=VMEM,
        out_shape=jax.ShapeDtypeStruct((QUERIES, 2 * HALF), bf16),
        scratch_shapes=[pltpu.VMEM((2 * HALF, QUERIES), f32)],
        compiler_params=SMALL,
        name="query_grads",
    )(inner, own, other, scale)


def share_kernel(terms_ref, out_ref):
    total = terms_ref[0].astype(f32)
    for y in range(1, NY):
        total += terms_ref[y].astype(f32)
    share = total.astype(bf16)
    for y in range(NY * ZH):
        out_ref[y] = share


def spread_share(terms):
    return pl.pallas_call(
        share_kernel,
        in_specs=[VMEM],
        out_specs=VMEM,
        out_shape=jax.ShapeDtypeStruct((NY * ZH, *terms.shape[1:]), bf16),
        compiler_params=SMALL,
        name="spread_share",
    )(terms)


def terms_kernel(late_ref, scaled_ref, other_ref, *refs):
    own, out_ref = refs[:ZL], refs[ZL]
    zl = late_ref[0]
    for k in range(ZL):
        terms = jnp.zeros((QUERIES, other_ref.shape[3]), f32)
        for h in range(ZH):
            terms += jnp.dot(scaled_ref[h, :, :HALF], own[k][0, h], preferred_element_type=f32)
            terms += jnp.dot(scaled_ref[h, :, HALF:], other_ref[k, h], preferred_element_type=f32)
        out_ref[zl ^ k] = terms.astype(bf16).reshape(NF, QUERIES // NF, terms.shape[1])


def score_terms(late, scaled, own, other):
    return pl.pallas_call(
        terms_kernel,
        in_specs=[SMEM] + [VMEM] * (2 + ZL),
        out_specs=VMEM,
        out_shape=jax.ShapeDtypeStruct((ZL, NF, QUERIES // NF, other.shape[3]), bf16),
        compiler_params=SMALL,
        name="score_terms",
    )(late, scaled, other, *own)


def late_kernel(place_ref, out_ref):
    for i in range(out_ref.shape[0]):
        out_ref[i] = place_ref[i]


def late_place(place):
    return pl.pallas_call(
        late_kernel,
        in_specs=[SMEM],
        out_specs=SMEM,
        out_shape=jax.ShapeDtypeStruct(place.shape, place.dtype),
        name="late_place",
    )(place)


def local(acts, out_grads, proj_in, proj_out, assignment, codes, zero_points, scales):
    flip = [(0, 1), (1, 0)]
    keep, send = project(acts, out_grads, proj_in, proj_out)
    got = lax.ppermute(send, "c", flip)
    parts = ((keep + got) * LINK_GAIN).astype(f16)
    parts = exchange(parts, ("yl", "x"))
    sums = jnp.sum(parts.astype(f32), axis=0)

    inner, packed = pack_tokens(sums, assignment)
    own = exchange(packed, ("zl", "zh"))
    swap = [(r * NW + w, w * NW + r) for r in range(NZ) for w in range(NW)]
    inner = lax.ppermute(inner, ("zl", "zh", "yl", "x"), swap)
    inner = exchange(jnp.broadcast_to(inner[None], (NW, *inner.shape)), ("yl", "x"))
    other = lax.ppermute(own, "c", flip)

    store = list(store_levels(codes, zero_points))
    for k in range(1, ZL):
        store[k] = lax.ppermute(store[k], "zl", [(r, r ^ k) for r in range(ZL)])
    store_other = lax.ppermute(jnp.stack([block[1] for block in store]), "c", flip)

    own_scale, other_scale = pick_scales(scales)
    other_scale = lax.ppermute(other_scale, "c", flip)
    scale = jnp.concatenate([own_scale, other_scale], axis=0).reshape(1, 2 * HALF)

    late = late_place(lax.axis_index("zl").reshape(1).astype(jnp.int32))
    grads = query_grads(inner, own, other, scale)
    grads = exchange(grads.reshape(NY, QUERIES // NY, 2 * HALF), "yh")
    scaled = exchange(spread_share(grads), ("zh", "yh")).reshape(ZH, QUERIES, 2 * HALF)

    terms = score_terms(late, scaled, store, store_other)
    terms = exchange(terms.reshape(ZL * NF, QUERIES // NF, codes.shape[0]), ("zl", "yl", "x", "c"))
    return jnp.sum(terms.astype(f32), axis=0)


def solution(mesh):
    split = Mesh(mesh.devices.reshape(4, 4, 2, 2, 4, 2), AXES)
    in_specs = (
        P(ROWS, FEAT),
        P(ROWS, FEAT),
        P(FEAT, None),
        P(FEAT, None),
        P(ROWS),
        P(ROWS, FEAT),
        P(FEAT),
        P(FEAT),
    )
    out_specs = P(FEAT, ROWS)
    return jax.shard_map(local, mesh=split, in_specs=in_specs, out_specs=out_specs, check_vma=False)
```
